256 devices in a mesh: row: 16 (over x, z_lo), col: 16 (over y, z_hi, core).
Axes of the slice: x: 4, y: 4, z: 8 (z_hi: 2, z_lo: 4; z = z_hi * 4 + z_lo), core: 2. Of those that a mesh axis runs over, the one named last changes fastest.
Arguments:
- t2_amps: bfloat16 [16384, 49152], P('row', 'col'), may hold values from -0.5 to 0.5
- l2_amps: bfloat16 [512, 49152], P('row', 'col'), may hold values from -0.02734375 to 0.02734375
Outputs:
- ladder: bfloat16 [512, 49152], P('row', 'col')
The draws below stay inside these ranges and needn't reach their ends.
All inputs are finite; a program needn't handle non-finite values.
Results may differ from the reference program's by a relative error of at most 0.0044.
Values may be sent and summed in bfloat16 or wider, within the bound.
A program may use at most 64 MiB of HBM per device.

```python
import jax
import jax.numpy as jnp

O = 128
OO = 16384
PV = 49152
KL = 512


def block_levels(own_key, shape, shards, low, largest):
    def one(position, parts):
        draws = jax.random.uniform(jax.random.fold_in(jax.random.fold_in(own_key, 6), position), (parts,), jnp.float32, low / len(shards), largest / len(shards))
        return jnp.repeat(jnp.exp(draws), shape[position] // parts).reshape((-1,) + (1,) * (len(shape) - position - 1))

    factor_of = one(*shards[0])
    for cut in shards[1:]:
        factor_of = factor_of * one(*cut)
    return factor_of


def gaussian(key, extent, width, most, cuts=(), kind=jnp.bfloat16):
    values = jax.random.normal(key, extent, jnp.float32) * width
    if len(cuts) > 0:
        values = block_levels(key, extent, cuts, -0.22, 0.18) * values
    return jnp.clip(values, min=-most, max=most).astype(kind)


def setup_inputs(seed: int = 0) -> dict:
    splits = jax.random.split(jax.random.key(seed), 3)
    return {
        "t2_amps": gaussian(splits[0], (OO, PV), O ** -0.5, 0.5, ((0, 16), (1, 16))),
        "l2_amps": gaussian(splits[1], (KL, PV), PV ** -0.5, 0.02734375, ((0, 16), (1, 16))),
    }


def reference(t2_amps, l2_amps):
    oooo = jnp.dot(t2_amps, l2_amps.T, preferred_element_type=jnp.float32)
    oooo_half = oooo.astype(jnp.bfloat16)
    ladder = jnp.dot(oooo_half.T, t2_amps, preferred_element_type=jnp.float32)
    return ladder.astype(jnp.bfloat16)
```

```python
import jax
import jax.numpy as jnp
from jax import lax
from jax.experimental import pallas as pl
from jax.experimental.pallas import tpu as pltpu
from jax.sharding import PartitionSpec as P

MESH = pl.DeviceIdType.MESH
F32, BF16 = jnp.float32, jnp.bfloat16

PARTS = 4
NX, NZ, NY = 4, 4, 4
STEP = 6.3
Z_TYPE = F32
R_TYPE = BF16


def kernel(
    t2_hbm, l2_hbm, out_ref,
    t2, g, p, rc, sy, ry, q, sz, rz, h, lad, xas, xa, xbs, xb, zs, zb,
    local, sems,
):
    rows, width = t2.shape
    piece = g.shape[2]
    row, col = lax.axis_index("row"), lax.axis_index("col")
    x, z = row // NZ, row % NZ
    y, zh, c = col // 4, (col // 2) % 2, col % 2

    def z_peer(d):
        return (x * NZ + (z + d) % NZ, col)

    def x_peer(d):
        return (((x + d) % NX) * NZ + z, col)

    def y_peer(d):
        return (row, ((y + d) % NY) * 4 + zh * 2 + c)

    far = (row, y * 4 + (1 - zh) * 2 + c)
    partner = (row, y * 4 + zh * 2 + (1 - c))

    load_t2 = pltpu.make_async_copy(t2_hbm, t2, local.at[0])
    load_t2.start()
    loads = []
    for j in range(PARTS):
        load = pltpu.make_async_copy(l2_hbm.at[pl.ds(j * piece, piece)], g.at[j, row], local.at[1 + j])
        load.start()
        loads.append(load)

    barrier = pltpu.get_barrier_semaphore()
    peers = [z_peer(1), z_peer(2), z_peer(3), x_peer(1), x_peer(3), y_peer(1), y_peer(2), y_peer(3), far, partner]
    for peer in peers:
        pl.semaphore_signal(barrier, inc=1, device_id=peer, device_id_type=MESH)
    pl.semaphore_wait(barrier, len(peers))

    names = {}
    sent = []

    def slot(name):
        return names.setdefault(name, len(names))

    def send(name, src, dst, device):
        k = slot(name)
        copy = pltpu.make_async_remote_copy(
            src_ref=src, dst_ref=dst, send_sem=sems.at[0, k], recv_sem=sems.at[1, k],
            device_id=device, device_id_type=MESH,
        )
        copy.start()
        sent.append(copy)

    def arrived(name, dst):
        k = slot(name)
        pltpu.make_async_remote_copy(
            src_ref=dst, dst_ref=dst, send_sem=sems.at[0, k], recv_sem=sems.at[1, k],
            device_id=partner, device_id_type=MESH,
        ).wait_recv()

    events = []

    def at(time):
        def add(f):
            events.append((time, len(events), f))
            return f

        return add

    def x_own(j):
        own = g.at[j, row]
        send(("x", j, 0, 0), own, own, x_peer(1))
        send(("x", j, 1, 0), own, own, x_peer(3))

    def chunk(j):
        base = j * STEP

        @at(0.0 + 0.001 * j)
        def _():
            loads[j].wait()
            own = g.at[j, row]
            if j == 0:
                x_own(j)
            for d in (1, 3, 2):
                send(("z", j, d), own, own, z_peer(d))

        @at(4.0 + base)
        def _():
            for d in (1, 3, 2):
                got = g.at[j, x * NZ + (z + NZ - d) % NZ]
                arrived(("z", j, d), got)
                send(("x", j, 0, d), got, got, x_peer(1))
                send(("x", j, 1, d), got, got, x_peer(3))
            if j + 1 < PARTS:
                x_own(j + 1)

        @at(8.0 + base)
        def _():
            for way, d in ((0, NX - 1), (1, 1)):
                group = ((x + d) % NX) * NZ
                for e in range(NZ):
                    arrived(("x", j, way, e), g.at[j, group + (z + NZ - e) % NZ])
                half = g.at[j, pl.ds(group + way * (NZ // 2), NZ // 2)]
                send(("relay", j, way), half, half, x_peer(1 if way == 0 else 3))

        m = 11.0 + base

        @at(m)
        def _():
            if j == 0:
                load_t2.wait()
            group = ((x + 2) % NX) * NZ
            for way in range(2):
                arrived(("relay", j, way), g.at[j, pl.ds(group + way * (NZ // 2), NZ // 2)])
            block = 256

            def one(n, _):
                at_n = pl.ds(pl.multiple_of(n * block, block), block)
                p[j, :, at_n] = lax.dot_general(
                    g[j].reshape(NX * NZ * piece, width), t2[at_n, :], (((1,), (1,)), ((), ())),
                    preferred_element_type=F32,
                )
                return _

            lax.fori_loop(0, rows // block, one, 0)
            half = p.shape[1] // 2
            send(("core", j), p.at[j, pl.ds((1 - c) * half, half)], rc.at[j], partner)

        @at(m + 3.5)
        def _():
            arrived(("core", j), rc.at[j])
            half = p.shape[1] // 2
            sy[j] = p[j, pl.ds(c * half, half), :] + rc[j]
            part = half // NY
            for d in (1, 3, 2):
                send(("y", j, d), sy.at[j, pl.ds(((y + d) % NY) * part, part)], ry.at[j, d - 1], y_peer(d))

        @at(m + 10.0)
        def _():
            part = q.shape[1]
            for d in (1, 3, 2):
                arrived(("y", j, d), ry.at[j, d - 1])
            total = sy[j, pl.ds(y * part, part), :] + ry[j, 0] + ry[j, 1] + ry[j, 2]
            q[j] = total
            sz[j] = total.astype(sz.dtype)
            send(("far", j), sz.at[j], rz.at[j], far)

        @at(m + 16.0)
        def _():
            part = q.shape[1]
            arrived(("far", j), rz.at[j])
            mine = pl.ds(c * (part * NY) + y * part, part)
            h[j, mine, :] = (q[j] + rz[j].astype(F32)).astype(BF16)
            own = h.at[j, mine]
            for d in (1, 3, 2):
                send(("ya", j, d), own, own, y_peer(d))

        @at(m + 20.0)
        def _():
            part = q.shape[1]
            for d in (1, 3, 2):
                arrived(("ya", j, d), h.at[j, pl.ds(c * (part * NY) + ((y + NY - d) % NY) * part, part)])
            own = h.at[j, pl.ds(c * (part * NY), part * NY)]
            send(("ca", j), own, own, partner)

        group_rows = NZ * piece
        half_rows = group_rows // 2

        def ladder_rows(group, half):
            return lad[j, pl.ds((group % NX) * group_rows + half * half_rows, half_rows), :]

        @at(m + 22.0)
        def _():
            part = q.shape[1]
            arrived(("ca", j), h.at[j, pl.ds((1 - c) * (part * NY), part * NY)])
            block = 512

            def one(n, _):
                at_n = pl.ds(pl.multiple_of(n * block, block), block)
                lad[j, :, at_n] = jnp.dot(h[j], t2[:, at_n], preferred_element_type=F32)
                return _

            lax.fori_loop(0, width // block, one, 0)
            for way in range(2):
                xas[j, way] = ladder_rows(x + 2, way).astype(BF16)
                send(("a", j, way), xas.at[j, way], xa.at[j, way], x_peer(1 if way == 0 else 3))
            for way in range(2):
                free = 1 - way
                xbs[j, way, free] = ladder_rows(x + (1 if way == 0 else 3), free).astype(BF16)
                send(("b", j, way, free), xbs.at[j, way, free], xb.at[j, way, free], x_peer(1 if way == 0 else 3))

        @at(m + 28.0)
        def _():
            for way in range(2):
                arrived(("a", j, way), xa.at[j, way])
                rows_ = ladder_rows(x + (1 if way == 0 else 3), way) + xa[j, way].astype(F32)
                xbs[j, way, way] = rows_.astype(BF16)
                send(("b", j, way, way), xbs.at[j, way, way], xb.at[j, way, way], x_peer(1 if way == 0 else 3))

        @at(m + 33.0)
        def _():
            for half in range(2):
                for way in range(2):
                    arrived(("b", j, way, half), xb.at[j, way, half])
                total = ladder_rows(x, half) + xb[j, 0, half].astype(F32) + xb[j, 1, half].astype(F32)
                lad[j, pl.ds(x * group_rows + half * half_rows, half_rows), :] = total
                for e in range(NZ // 2):
                    zs[j, half * (NZ // 2) + e] = total[e * piece : (e + 1) * piece].astype(zs.dtype)
            for d in (2, 1, 3):
                send(("zr", j, d), zs.at[j, (z + d) % NZ], zb.at[j, d - 1], z_peer(d))

        @at(m + 41.0)
        def _():
            for d in (1, 3, 2):
                arrived(("zr", j, d), zb.at[j, d - 1])
            total = lad[j, pl.ds(x * group_rows + z * piece, piece), :]
            for d in range(3):
                total += zb[j, d].astype(F32)
            out_ref[pl.ds(j * piece, piece), :] = total.astype(BF16)

    for j in range(PARTS):
        chunk(j)
    for _, _, event in sorted(events, key=lambda e: e[:2]):
        event()
    for copy in sent:
        copy.wait_send()


def on_device(t2_amps, l2_amps):
    rows, width = t2_amps.shape
    piece = l2_amps.shape[0] // PARTS
    kl = NX * NZ * piece
    part = kl // 2 // NY
    half = NZ * piece // 2
    return pl.pallas_call(
        kernel,
        out_shape=jax.ShapeDtypeStruct(l2_amps.shape, BF16),
        in_specs=[pl.BlockSpec(memory_space=pl.ANY)] * 2,
        out_specs=pl.BlockSpec(memory_space=pltpu.VMEM),
        scratch_shapes=[
            pltpu.VMEM((rows, width), BF16),
            pltpu.VMEM((PARTS, NX * NZ, piece, width), BF16),
            pltpu.VMEM((PARTS, kl, rows), F32),
            pltpu.VMEM((PARTS, kl // 2, rows), F32),
            pltpu.VMEM((PARTS, kl // 2, rows), F32),
            pltpu.VMEM((PARTS, NY - 1, part, rows), F32),
            pltpu.VMEM((PARTS, part, rows), F32),
            pltpu.VMEM((PARTS, part, rows), Z_TYPE),
            pltpu.VMEM((PARTS, part, rows), Z_TYPE),
            pltpu.VMEM((PARTS, kl, rows), BF16),
            pltpu.VMEM((PARTS, kl, width), F32),
            pltpu.VMEM((PARTS, 2, half, width), BF16),
            pltpu.VMEM((PARTS, 2, half, width), BF16),
            pltpu.VMEM((PARTS, 2, 2, half, width), BF16),
            pltpu.VMEM((PARTS, 2, 2, half, width), BF16),
            pltpu.VMEM((PARTS, NZ, piece, width), R_TYPE),
            pltpu.VMEM((PARTS, NZ - 1, piece, width), R_TYPE),
            pltpu.SemaphoreType.DMA((1 + PARTS,)),
            pltpu.SemaphoreType.DMA((2, 31 * PARTS)),
        ],
        compiler_params=pltpu.CompilerParams(
            collective_id=0, has_side_effects=True, vmem_limit_bytes=60 * 2**20
        ),
    )(t2_amps, l2_amps)


def solution(mesh):
    return jax.shard_map(
        on_device,
        mesh=mesh,
        in_specs=(P("row", "col"), P("row", "col")),
        out_specs=P("row", "col"),
        check_vma=False,
    )
```

```python
import jax
import jax.numpy as jnp
from jax import lax
from jax.experimental import pallas as pl
from jax.experimental.pallas import tpu as pltpu
from jax.sharding import PartitionSpec as P

MESH = pl.DeviceIdType.MESH
F32, BF16 = jnp.float32, jnp.bfloat16

PARTS = 4
CHUNKS = 2 * PARTS
NX, NZ, NY = 4, 4, 4
FAR_TYPE = BF16

ORDER = (
    "ob0 ox1 ox0 ox3",
    "oa0 f10 oa1 f30",
    "tt1 tt3 ox2 ob1",
    "tt0 f20 rl1 oa2",
    "tt2 f21 rl0 f31",
    "f11 ob2 ma1 rl2",
    "ys1 oa3 f22 ma0",
    "rl3 f32 ys0 ob3",
    "f12 ma2 rl4 yq1",
    "ys2 f23 ma3 yq0",
    "rl5 f13 f33 ys3",
    "ma4 rl6 yq2 zq1",
    "ys4 ma5 zq0 yq3",
    "rl7 ys5 ma6 zq2",
    "ca1 yq4 ys6 ca0",
    "ma7 mm0 ys7 yq5",
    "ca2 zq3 bf0 mm1",
    "mm2 yq6 zq4 bf2",
    "bd0 yq7 bf1 ca3",
    "zq5 bd1 ca4 bd2",
    "mm3 mm4 bs0 bf4",
    "zq6 ca5 zq7 bf3",
    "bs1 bd3 mm5 bd4",
    "bf5 ca6 ca7 bs2",
    "mm6 mm7 bs4 bd5",
    "ou0 bs3 bf6 bd6",
    "bf7 bs5 bd7 bs6",
    "bs7 ou2 ou1 ou3",
)


def kernel(
    t2_hbm, l2_hbm, out_hbm,
    t2, t2t, g, p, rc, sy, ry, q, sz, rz, h, lad, xas, xa, xbs, xb, zs, zb, out,
    local, send_sems, sems,
):
    rows, width = t2.shape
    piece = g.shape[3]
    kl = p.shape[1]
    half = kl // 2
    row, col = lax.axis_index("row"), lax.axis_index("col")
    x, z = row // NZ, row % NZ
    zz = z // 2
    y, zh, c = col // 4, (col // 2) % 2, col % 2

    def z_peer(d):
        return (x * NZ + (z + d) % NZ, col)

    def x_peer(way):
        return (((x + (1 if way == 0 else NX - 1)) % NX) * NZ + z, col)

    def y_peer(d):
        return (row, ((y + d) % NY) * 4 + zh * 2 + c)

    far = (row, y * 4 + (1 - zh) * 2 + c)
    partner = (row, y * 4 + zh * 2 + (1 - c))

    loads = []
    for j in range(PARTS):
        loads.append(pltpu.make_async_copy(l2_hbm.at[pl.ds(j * piece, piece)], g.at[2 * j, x, zz], local.at[j]))
    loads.append(pltpu.make_async_copy(t2_hbm, t2, local.at[PARTS]))
    for copy in loads:
        copy.start()

    barrier = pltpu.get_barrier_semaphore()
    peers = [z_peer(1), z_peer(2), z_peer(3), x_peer(0), x_peer(1), y_peer(1), y_peer(2), y_peer(3), far, partner]
    for peer in peers:
        pl.semaphore_signal(barrier, inc=1, device_id=peer, device_id_type=MESH)
    pl.semaphore_wait(barrier, len(peers))

    names = {}

    count = [0]

    def index(name, size=1):
        if name not in names:
            names[name] = count[0]
            count[0] += size
        return names[name]

    kinds = ("x", "z", "c", "y", "far", "ya", "ca", "a", "b", "zr")

    def send(kind, k, src, dst, device):
        pltpu.make_async_remote_copy(
            src_ref=src, dst_ref=dst, send_sem=send_sems.at[kinds.index(kind)], recv_sem=sems.at[k],
            device_id=device, device_id_type=MESH,
        ).start()

    def waiting(kind, k, ref):
        return pltpu.make_async_remote_copy(
            src_ref=ref, dst_ref=ref, send_sem=send_sems.at[kinds.index(kind)], recv_sem=sems.at[k],
            device_id=partner, device_id_type=MESH,
        )

    def arrived(k, ref):
        with jax.named_scope("w"):
            waiting("x", k, ref).wait_recv()

    def send_x(k, slot_z):
        block = g.at[k, x, slot_z]
        first = index(("x", k), 3)
        for way in range(2):
            send("x", first + jnp.where(slot_z == way, way, 2), block, block, x_peer(way))

    loaded = set()

    def load(j):
        if j not in loaded:
            loaded.add(j)
            loads[j].wait()

    def to_z(j, d):
        load(j)
        send("z", index(("z", j, d)), g.at[2 * j, x, zz], g.at[2 * j + d % 2, x, zz], z_peer(d))

    def oa(j):
        to_z(j, 2)

    def ob(j):
        to_z(j, 1)
        to_z(j, 3)

    def ox(j):
        load(j)
        send_x(2 * j, zz)

    def from_z(j, d):
        k, slot_z = 2 * j + d % 2, ((z + NZ - d) % NZ) // 2
        arrived(index(("z", j, d)), g.at[k, x, slot_z])
        send_x(k, slot_z)

    def f1(j):
        from_z(j, 1)

    def f2(j):
        from_z(j, 2)

    def f3(j):
        from_z(j, 3)

    def rl(k):
        for way in range(2):
            block = g.at[k, (x + (NX - 1 if way == 0 else 1)) % NX, way]
            arrived(index(("x", k), 3) + way, block)
            send("x", index(("x", k), 3) + 2, block, block, x_peer(way))

    def ma(k):
        arrived(index(("x", k), 3) + 2, g.at[k, pl.ds(0, 2)])
        columns = rows // 2
        for s in range(2):
            at_s = pl.ds(s * columns, columns)
            p[k, :, at_s] = jnp.dot(g[k].reshape(kl, width), t2t[:, at_s], preferred_element_type=F32)
            send("c", index(("c", k)), p.at[k, pl.ds((1 - c) * half, half), at_s], rc.at[k, :, at_s], partner)

    def tt(i):
        load(PARTS)
        size = rows // 4
        t2t[:, i * size : (i + 1) * size] = t2[i * size : (i + 1) * size, :].T

    def ys(k):
        arrived(index(("c", k)), rc.at[k])
        sy[k] = (p[k, pl.ds(c * half, half), :] + rc[k]).reshape(NY, half // NY, rows)
        for d in (2, 1, 3):
            send("y", index(("y", k)), sy.at[k, (y + d) % NY], ry.at[k, d - 1], y_peer(d))

    def yq(k):
        arrived(index(("y", k)), ry.at[k])
        total = sy[k, y] + ry[k, 0] + ry[k, 1] + ry[k, 2]
        q[k] = total
        sz[k] = total.astype(sz.dtype)
        send("far", index(("far", k)), sz.at[k], rz.at[k], far)

    def zq(k):
        arrived(index(("far", k)), rz.at[k])
        h[k, c, y] = (q[k] + rz[k].astype(F32)).astype(BF16)
        own = h.at[k, c, y]
        for d in (2, 1, 3):
            send("ya", index(("ya", k)), own, own, y_peer(d))

    def ca(k):
        arrived(index(("ya", k)), h.at[k, c, pl.ds(0, NY - 1)])
        own = h.at[k, c]
        send("ca", index(("ca", k)), own, own, partner)

    def ladder_rows(k, group, slot_z):
        return lad[k, pl.ds((group % NX) * (2 * piece) + slot_z * piece, piece), :]

    def mm(k):
        arrived(index(("ca", k)), h.at[k, 1 - c])
        lad[k] = jnp.dot(h[k].reshape(kl, rows), t2[...], preferred_element_type=F32)
        for way in range(2):
            xas[k, way] = ladder_rows(k, x + 2, way).astype(BF16)
            send("a", index(("a", k, way)), xas.at[k, way], xa.at[k, way], x_peer(way))

    def bf(k):
        for way in range(2):
            xbs[k, 1 - way, way] = ladder_rows(k, x + (1 if way == 0 else 3), 1 - way).astype(BF16)
            send("b", index(("b", k, 1 - way)), xbs.at[k, 1 - way, way], xb.at[k, 1 - way, way], x_peer(way))

    def bd(k):
        for way in range(2):
            arrived(index(("a", k, way)), xa.at[k, way])
            total = ladder_rows(k, x + (1 if way == 0 else 3), way) + xa[k, way].astype(F32)
            xbs[k, way, way] = total.astype(BF16)
            send("b", index(("b", k, way)), xbs.at[k, way, way], xb.at[k, way, way], x_peer(way))

    def bs(k):
        for slot_z in range(2):
            arrived(index(("b", k, slot_z)), xb.at[k, slot_z])
            total = ladder_rows(k, x, slot_z) + xb[k, slot_z, 0].astype(F32) + xb[k, slot_z, 1].astype(F32)
            if k % 2 == 0:
                lad[k, pl.ds(x * (2 * piece) + slot_z * piece, piece), :] = total
            zs[k, slot_z] = total.astype(BF16)
        for d in (2,) if k % 2 == 0 else (1, 3):
            send("zr", index(("zr", k // 2)), zs.at[k, ((z + d) % NZ) // 2], zb.at[k // 2, d - 1], z_peer(d))

    stores = []

    def ou(j):
        arrived(index(("zr", j)), zb.at[j])
        total = ladder_rows(2 * j, x, zz)
        for d in range(3):
            total += zb[j, d].astype(F32)
        out[j] = total.astype(BF16)
        store = pltpu.make_async_copy(out.at[j], out_hbm.at[pl.ds(j * piece, piece)], local.at[j])
        store.start()
        stores.append(store)

    events = dict(oa=oa, ob=ob, tt=tt, ox=ox, f1=f1, f2=f2, f3=f3, rl=rl, ma=ma, ys=ys, yq=yq, zq=zq, ca=ca, mm=mm, bf=bf, bd=bd, bs=bs, ou=ou)
    for name in " ".join(ORDER).split():
        with jax.named_scope(name):
            events[name[:2]](int(name[2:]))
    with jax.named_scope("drain"):
        sent = dict(
            x=g.at[pl.ds(0, 6)], z=zb, c=rc, y=ry, far=rz, ya=h.at[pl.ds(0, 3)], ca=h.at[pl.ds(0, 4)], a=xa, b=xb, zr=zb
        )
        for kind in kinds:
            waiting(kind, 0, sent[kind]).wait_send()
        for store in stores:
            store.wait()


def on_device(t2_amps, l2_amps):
    rows, width = t2_amps.shape
    piece = l2_amps.shape[0] // PARTS
    kl = NX * 2 * piece
    return pl.pallas_call(
        kernel,
        out_shape=jax.ShapeDtypeStruct(l2_amps.shape, BF16),
        in_specs=[pl.BlockSpec(memory_space=pl.ANY)] * 2,
        out_specs=pl.BlockSpec(memory_space=pl.ANY),
        scratch_shapes=[
            pltpu.VMEM((rows, width), BF16),
            pltpu.VMEM((width, rows), BF16),
            pltpu.VMEM((CHUNKS, NX, 2, piece, width), BF16),
            pltpu.VMEM((CHUNKS, kl, rows), F32),
            pltpu.VMEM((CHUNKS, kl // 2, rows), F32),
            pltpu.VMEM((CHUNKS, NY, kl // 2 // NY, rows), F32),
            pltpu.VMEM((CHUNKS, NY - 1, kl // 2 // NY, rows), F32),
            pltpu.VMEM((CHUNKS, kl // 2 // NY, rows), F32),
            pltpu.VMEM((CHUNKS, kl // 2 // NY, rows), FAR_TYPE),
            pltpu.VMEM((CHUNKS, kl // 2 // NY, rows), FAR_TYPE),
            pltpu.VMEM((CHUNKS, 2, NY, kl // 2 // NY, rows), BF16),
            pltpu.VMEM((CHUNKS, kl, width), F32),
            pltpu.VMEM((CHUNKS, 2, piece, width), BF16),
            pltpu.VMEM((CHUNKS, 2, piece, width), BF16),
            pltpu.VMEM((CHUNKS, 2, 2, piece, width), BF16),
            pltpu.VMEM((CHUNKS, 2, 2, piece, width), BF16),
            pltpu.VMEM((CHUNKS, 2, piece, width), BF16),
            pltpu.VMEM((PARTS, NZ - 1, piece, width), BF16),
            pltpu.VMEM((PARTS, piece, width), BF16),
            pltpu.SemaphoreType.DMA((1 + PARTS,)),
            pltpu.SemaphoreType.DMA((10,)),
            pltpu.SemaphoreType.DMA((CHUNKS * 14,)),
        ],
        compiler_params=pltpu.CompilerParams(
            collective_id=0, has_side_effects=True, vmem_limit_bytes=60 * 2**20
        ),
    )(t2_amps, l2_amps)


def solution(mesh):
    return jax.shard_map(
        on_device,
        mesh=mesh,
        in_specs=(P("row", "col"), P("row", "col")),
        out_specs=P("row", "col"),
        check_vma=False,
    )
```

```python
import jax
import jax.numpy as jnp
from jax import lax
from jax.experimental import pallas as pl
from jax.experimental.pallas import tpu as pltpu
from jax.sharding import PartitionSpec as P

MESH = pl.DeviceIdType.MESH
F32, BF16 = jnp.float32, jnp.bfloat16

PARTS = 4
CHUNKS = 2 * PARTS
NX, NZ, NY = 4, 4, 4
FAR_TYPE = BF16

ORDER = (
    "ob0 ox0 ox1 ox3",
    "oa0 tt1 f10 ob1",
    "f30 ox2 tt3 oa1",
    "tt0 f20 rl1 oa2",
    "f11 tt2 f31 rl0",
    "f21 ob2 ma1 rl3",
    "f22 oa3 ys1 ma0",
    "rl2 f12 ob3 f32",
    "ys0 ma3 yq1 rl4",
    "ys3 f23 ma2 yq0",
    "rl5 f33 ys2 ma4",
    "zq1 yq3 rl6 f13",
    "ys4 ma5 yq2 zq0",
    "ca1 ys5 ma6 rl7",
    "yq4 mm1 ca0 zq3",
    "ys6 bf1 mm0 yq5",
    "zq2 bf0 ma7 bd1",
    "ca3 zq4 ys7 yq6",
    "bd0 mm3 ca2 bf3",
    "zq5 ca4 mm2 yq7",
    "bf2 mm4 zq6 ca5",
    "bs1 bd3 bd2 mm5",
    "ca6 bf4 zq7 bs3",
    "bd4 mm6 bs2 bf5",
    "bf6 bd5 ca7 bs4",
    "bs0 mm7 bd6 bf7",
    "bs5 bd7 ou1 bs6",
    "bs7 ou0 ou2 ou3",
)


def kernel(
    t2_hbm, l2_hbm, out_hbm,
    t2, t2t, g, p, rc, sy, ry, q, sz, rz, h, lad, xas, xa, xbs, xb, zs, zb, out,
    local, send_sems, sems,
):
    rows, width = t2.shape
    piece = g.shape[3]
    kl = p.shape[1]
    half = kl // 2
    row, col = lax.axis_index("row"), lax.axis_index("col")
    x, z = row // NZ, row % NZ
    zz = z // 2
    y, zh, c = col // 4, (col // 2) % 2, col % 2

    def z_peer(d):
        return (x * NZ + (z + d) % NZ, col)

    def x_peer(way):
        return (((x + (1 if way == 0 else NX - 1)) % NX) * NZ + z, col)

    def y_peer(d):
        return (row, ((y + d) % NY) * 4 + zh * 2 + c)

    far = (row, y * 4 + (1 - zh) * 2 + c)
    partner = (row, y * 4 + zh * 2 + (1 - c))

    loads = []
    for j in range(PARTS):
        loads.append(pltpu.make_async_copy(l2_hbm.at[pl.ds(j * piece, piece)], g.at[2 * j, x, zz], local.at[j]))
    loads.append(pltpu.make_async_copy(t2_hbm, t2, local.at[PARTS]))
    for copy in loads:
        copy.start()

    barrier = pltpu.get_barrier_semaphore()
    peers = [z_peer(1), z_peer(2), z_peer(3), x_peer(0), x_peer(1), y_peer(1), y_peer(2), y_peer(3), far, partner]
    for peer in peers:
        pl.semaphore_signal(barrier, inc=1, device_id=peer, device_id_type=MESH)
    pl.semaphore_wait(barrier, len(peers))

    names = {}

    count = [0]

    def index(name, size=1):
        if name not in names:
            names[name] = count[0]
            count[0] += size
        return names[name]

    kinds = ("x", "z", "c", "y", "far", "ya", "ca", "a", "b", "zr")

    def send(kind, k, src, dst, device):
        pltpu.make_async_remote_copy(
            src_ref=src, dst_ref=dst, send_sem=send_sems.at[kinds.index(kind)], recv_sem=sems.at[k],
            device_id=device, device_id_type=MESH,
        ).start()

    def waiting(kind, k, ref):
        return pltpu.make_async_remote_copy(
            src_ref=ref, dst_ref=ref, send_sem=send_sems.at[kinds.index(kind)], recv_sem=sems.at[k],
            device_id=partner, device_id_type=MESH,
        )

    def arrived(k, ref):
        with jax.named_scope("w"):
            waiting("x", k, ref).wait_recv()

    def send_x(k, slot_z):
        block = g.at[k, x, slot_z]
        first = index(("x", k), 3)
        for way in range(2):
            send("x", first + jnp.where(slot_z == way, way, 2), block, block, x_peer(way))

    loaded = set()

    def load(j):
        if j not in loaded:
            loaded.add(j)
            loads[j].wait()

    def to_z(j, d):
        load(j)
        send("z", index(("z", j, d)), g.at[2 * j, x, zz], g.at[2 * j + d % 2, x, zz], z_peer(d))

    def oa(j):
        to_z(j, 2)

    def ob(j):
        to_z(j, 1)
        to_z(j, 3)

    def ox(j):
        load(j)
        send_x(2 * j, zz)

    def from_z(j, d):
        k, slot_z = 2 * j + d % 2, ((z + NZ - d) % NZ) // 2
        arrived(index(("z", j, d)), g.at[k, x, slot_z])
        send_x(k, slot_z)

    def f1(j):
        from_z(j, 1)

    def f2(j):
        from_z(j, 2)

    def f3(j):
        from_z(j, 3)

    def rl(k):
        for way in range(2):
            block = g.at[k, (x + (NX - 1 if way == 0 else 1)) % NX, way]
            arrived(index(("x", k), 3) + way, block)
            send("x", index(("x", k), 3) + 2, block, block, x_peer(way))

    def ma(k):
        arrived(index(("x", k), 3) + 2, g.at[k, pl.ds(0, 2)])
        columns = rows // 2
        for s in range(2):
            at_s = pl.ds(s * columns, columns)
            p[k, :, at_s] = jnp.dot(g[k].reshape(kl, width), t2t[:, at_s], preferred_element_type=F32)
            send("c", index(("c", k)), p.at[k, pl.ds((1 - c) * half, half), at_s], rc.at[k, :, at_s], partner)

    def tt(i):
        load(PARTS)
        size = rows // 4
        t2t[:, i * size : (i + 1) * size] = t2[i * size : (i + 1) * size, :].T

    def ys(k):
        arrived(index(("c", k)), rc.at[k])
        sy[k] = (p[k, pl.ds(c * half, half), :] + rc[k]).reshape(NY, half // NY, rows)
        for d in (2, 1, 3):
            send("y", index(("y", k)), sy.at[k, (y + d) % NY], ry.at[k, d - 1], y_peer(d))

    def yq(k):
        arrived(index(("y", k)), ry.at[k])
        total = sy[k, y] + ry[k, 0] + ry[k, 1] + ry[k, 2]
        q[k] = total
        sz[k] = total.astype(sz.dtype)
        send("far", index(("far", k)), sz.at[k], rz.at[k], far)

    def zq(k):
        arrived(index(("far", k)), rz.at[k])
        h[k, c, y] = (q[k] + rz[k].astype(F32)).astype(BF16)
        own = h.at[k, c, y]
        for d in (2, 1, 3):
            send("ya", index(("ya", k)), own, own, y_peer(d))

    def ca(k):
        arrived(index(("ya", k)), h.at[k, c, pl.ds(0, NY - 1)])
        own = h.at[k, c]
        send("ca", index(("ca", k)), own, own, partner)

    def ladder_rows(k, group, slot_z):
        return lad[k, pl.ds((group % NX) * (2 * piece) + slot_z * piece, piece), :]

    def mm(k):
        arrived(index(("ca", k)), h.at[k, 1 - c])
        lad[k] = jnp.dot(h[k].reshape(kl, rows), t2[...], preferred_element_type=F32)
        for way in range(2):
            xas[k, way] = ladder_rows(k, x + 2, way).astype(BF16)
            send("a", index(("a", k, way)), xas.at[k, way], xa.at[k, way], x_peer(way))

    def bf(k):
        for way in range(2):
            xbs[k, 1 - way, way] = ladder_rows(k, x + (1 if way == 0 else 3), 1 - way).astype(BF16)
            send("b", index(("b", k, 1 - way)), xbs.at[k, 1 - way, way], xb.at[k, 1 - way, way], x_peer(way))

    def bd(k):
        for way in range(2):
            arrived(index(("a", k, way)), xa.at[k, way])
            total = ladder_rows(k, x + (1 if way == 0 else 3), way) + xa[k, way].astype(F32)
            xbs[k, way, way] = total.astype(BF16)
            send("b", index(("b", k, way)), xbs.at[k, way, way], xb.at[k, way, way], x_peer(way))

    def bs(k):
        for slot_z in range(2):
            arrived(index(("b", k, slot_z)), xb.at[k, slot_z])
            total = ladder_rows(k, x, slot_z) + xb[k, slot_z, 0].astype(F32) + xb[k, slot_z, 1].astype(F32)
            if k % 2 == 0:
                lad[k, pl.ds(x * (2 * piece) + slot_z * piece, piece), :] = total
            zs[k, slot_z] = total.astype(BF16)
        for d in (2,) if k % 2 == 0 else (1, 3):
            send("zr", index(("zr", k // 2)), zs.at[k, ((z + d) % NZ) // 2], zb.at[k // 2, d - 1], z_peer(d))

    stores = []

    def ou(j):
        arrived(index(("zr", j)), zb.at[j])
        total = ladder_rows(2 * j, x, zz)
        for d in range(3):
            total += zb[j, d].astype(F32)
        out[j] = total.astype(BF16)
        store = pltpu.make_async_copy(out.at[j], out_hbm.at[pl.ds(j * piece, piece)], local.at[j])
        store.start()
        stores.append(store)

    events = dict(oa=oa, ob=ob, tt=tt, ox=ox, f1=f1, f2=f2, f3=f3, rl=rl, ma=ma, ys=ys, yq=yq, zq=zq, ca=ca, mm=mm, bf=bf, bd=bd, bs=bs, ou=ou)
    for name in " ".join(ORDER).split():
        with jax.named_scope(name):
            events[name[:2]](int(name[2:]))
    with jax.named_scope("drain"):
        sent = dict(
            x=g.at[pl.ds(0, 6)], z=zb, c=rc, y=ry, far=rz, ya=h.at[pl.ds(0, 3)], ca=h.at[pl.ds(0, 4)], a=xa, b=xb, zr=zb
        )
        for kind in kinds:
            waiting(kind, 0, sent[kind]).wait_send()
        for store in stores:
            store.wait()


def on_device(t2_amps, l2_amps):
    rows, width = t2_amps.shape
    piece = l2_amps.shape[0] // PARTS
    kl = NX * 2 * piece
    return pl.pallas_call(
        kernel,
        out_shape=jax.ShapeDtypeStruct(l2_amps.shape, BF16),
        in_specs=[pl.BlockSpec(memory_space=pl.ANY)] * 2,
        out_specs=pl.BlockSpec(memory_space=pl.ANY),
        scratch_shapes=[
            pltpu.VMEM((rows, width), BF16),
            pltpu.VMEM((width, rows), BF16),
            pltpu.VMEM((CHUNKS, NX, 2, piece, width), BF16),
            pltpu.VMEM((CHUNKS, kl, rows), F32),
            pltpu.VMEM((CHUNKS, kl // 2, rows), F32),
            pltpu.VMEM((CHUNKS, NY, kl // 2 // NY, rows), F32),
            pltpu.VMEM((CHUNKS, NY - 1, kl // 2 // NY, rows), F32),
            pltpu.VMEM((CHUNKS, kl // 2 // NY, rows), F32),
            pltpu.VMEM((CHUNKS, kl // 2 // NY, rows), FAR_TYPE),
            pltpu.VMEM((CHUNKS, kl // 2 // NY, rows), FAR_TYPE),
            pltpu.VMEM((CHUNKS, 2, NY, kl // 2 // NY, rows), BF16),
            pltpu.VMEM((CHUNKS, kl, width), F32),
            pltpu.VMEM((CHUNKS, 2, piece, width), BF16),
            pltpu.VMEM((CHUNKS, 2, piece, width), BF16),
            pltpu.VMEM((CHUNKS, 2, 2, piece, width), BF16),
            pltpu.VMEM((CHUNKS, 2, 2, piece, width), BF16),
            pltpu.VMEM((CHUNKS, 2, piece, width), BF16),
            pltpu.VMEM((PARTS, NZ - 1, piece, width), BF16),
            pltpu.VMEM((PARTS, piece, width), BF16),
            pltpu.SemaphoreType.DMA((1 + PARTS,)),
            pltpu.SemaphoreType.DMA((10,)),
            pltpu.SemaphoreType.DMA((CHUNKS * 14,)),
        ],
        compiler_params=pltpu.CompilerParams(
            collective_id=0, has_side_effects=True, vmem_limit_bytes=60 * 2**20
        ),
    )(t2_amps, l2_amps)


def solution(mesh):
    return jax.shard_map(
        on_device,
        mesh=mesh,
        in_specs=(P("row", "col"), P("row", "col")),
        out_specs=P("row", "col"),
        check_vma=False,
    )
```

```python
import jax
import jax.numpy as jnp
from jax import lax
from jax.experimental import pallas as pl
from jax.experimental.pallas import tpu as pltpu
from jax.sharding import PartitionSpec as P

MESH = pl.DeviceIdType.MESH
F32, BF16 = jnp.float32, jnp.bfloat16

PARTS = 4
CHUNKS = 2 * PARTS
NX, NZ, NY = 4, 4, 4
FAR_TYPE = BF16

ORDER = (
    "ob1 ox2 ox0 ox1",
    "ob0 tt1 tt0 f11",
    "oa3 f31 f10 f30",
    "oa0 rl3 ox3 tt3",
    "oa1 f23 oa2 rl1",
    "tt2 f20 ma3 ob3",
    "rl6 f21 ys3 ma1",
    "rl0 ob2 f13 f22",
    "ys1 ma6 rl2 yq3",
    "ys6 f12 ma0 f32",
    "yq1 ys0 rl4 f33",
    "ma2 yq6 zq3 rl5",
    "ys2 ma4 yq0 zq1",
    "rl7 ca3 ys4 ma5",
    "yq2 zq6 mm3 ys5",
    "ca1 bf3 ma7 zq0",
    "mm1 yq4 ys7 bd3",
    "ca6 bf1 yq5 zq2",
    "mm6 bf6 bd1 ca0",
    "yq7 mm0 ca2 zq4",
    "bf0 mm2 bd6 zq5",
    "bf2 bd0 bs3 ca4",
    "zq7 mm4 bd2 bf4",
    "bs1 ca5 bs6 mm5",
    "ca7 bs0 bd4 mm7",
    "bs2 bf5 bd5 bs4",
    "bf7 bd7 bs5 ou1",
    "bs7 ou2 ou0 ou3",
)


def kernel(
    t2_hbm, l2_hbm, out_ref,
    t2, t2t, g, p, rc, sy, ry, q, sz, rz, h, lad, xas, xa, xbs, xb, zs, zb,
    local, send_sems, sems,
):
    rows, width = t2.shape
    piece = g.shape[3]
    kl = p.shape[1]
    half = kl // 2
    row, col = lax.axis_index("row"), lax.axis_index("col")
    x, z = row // NZ, row % NZ
    zz = z // 2
    y, zh, c = col // 4, (col // 2) % 2, col % 2

    def z_peer(d):
        return (x * NZ + (z + d) % NZ, col)

    def x_peer(way):
        return (((x + (1 if way == 0 else NX - 1)) % NX) * NZ + z, col)

    def y_peer(d):
        return (row, ((y + d) % NY) * 4 + zh * 2 + c)

    far = (row, y * 4 + (1 - zh) * 2 + c)
    partner = (row, y * 4 + zh * 2 + (1 - c))

    loads = []
    for j in range(PARTS):
        loads.append(pltpu.make_async_copy(l2_hbm.at[pl.ds(j * piece, piece)], g.at[2 * j, x, zz], local.at[j]))
    loads.append(pltpu.make_async_copy(t2_hbm, t2, local.at[PARTS]))
    for copy in loads:
        copy.start()

    barrier = pltpu.get_barrier_semaphore()
    peers = [z_peer(1), z_peer(2), z_peer(3), x_peer(0), x_peer(1), y_peer(1), y_peer(2), y_peer(3), far, partner]
    for peer in peers:
        pl.semaphore_signal(barrier, inc=1, device_id=peer, device_id_type=MESH)
    pl.semaphore_wait(barrier, len(peers))

    names = {}

    words = " ".join(ORDER).split()
    last = max(range(CHUNKS), key=lambda k: words.index(f"bs{k}"))
    count = [0]

    def cuts(k):
        n = 2 if k == last else 1
        return [pl.ds(s * (width // n), width // n) for s in range(n)]

    def index(name, size=1):
        if name not in names:
            names[name] = count[0]
            count[0] += size
        return names[name]

    kinds = ("x", "z", "c", "y", "far", "ya", "ca", "a", "b", "zr")

    def send(kind, k, src, dst, device):
        pltpu.make_async_remote_copy(
            src_ref=src, dst_ref=dst, send_sem=send_sems.at[kinds.index(kind)], recv_sem=sems.at[k],
            device_id=device, device_id_type=MESH,
        ).start()

    def waiting(kind, k, ref):
        return pltpu.make_async_remote_copy(
            src_ref=ref, dst_ref=ref, send_sem=send_sems.at[kinds.index(kind)], recv_sem=sems.at[k],
            device_id=partner, device_id_type=MESH,
        )

    def arrived(k, ref):
        with jax.named_scope("w"):
            waiting("x", k, ref).wait_recv()

    def send_x(k, slot_z):
        block = g.at[k, x, slot_z]
        first = index(("x", k), 3)
        for way in range(2):
            send("x", first + jnp.where(slot_z == way, way, 2), block, block, x_peer(way))

    loaded = set()

    def load(j):
        if j not in loaded:
            loaded.add(j)
            loads[j].wait()

    def to_z(j, d):
        load(j)
        send("z", index(("z", j, d)), g.at[2 * j, x, zz], g.at[2 * j + d % 2, x, zz], z_peer(d))

    def oa(j):
        to_z(j, 2)

    def ob(j):
        to_z(j, 1)
        to_z(j, 3)

    def ox(j):
        load(j)
        send_x(2 * j, zz)

    def from_z(j, d):
        k, slot_z = 2 * j + d % 2, ((z + NZ - d) % NZ) // 2
        arrived(index(("z", j, d)), g.at[k, x, slot_z])
        send_x(k, slot_z)

    def f1(j):
        from_z(j, 1)

    def f2(j):
        from_z(j, 2)

    def f3(j):
        from_z(j, 3)

    def rl(k):
        for way in range(2):
            block = g.at[k, (x + (NX - 1 if way == 0 else 1)) % NX, way]
            arrived(index(("x", k), 3) + way, block)
            send("x", index(("x", k), 3) + 2, block, block, x_peer(way))

    def ma(k):
        arrived(index(("x", k), 3) + 2, g.at[k, pl.ds(0, 2)])
        columns = rows // 2
        for s in range(2):
            at_s = pl.ds(s * columns, columns)
            p[k, :, at_s] = jnp.dot(g[k].reshape(kl, width), t2t[:, at_s], preferred_element_type=F32)
            send("c", index(("c", k)), p.at[k, pl.ds((1 - c) * half, half), at_s], rc.at[k, :, at_s], partner)

    def tt(i):
        load(PARTS)
        size = rows // 4
        t2t[:, i * size : (i + 1) * size] = t2[i * size : (i + 1) * size, :].T

    def ys(k):
        arrived(index(("c", k)), rc.at[k])
        sy[k] = (p[k, pl.ds(c * half, half), :] + rc[k]).reshape(NY, half // NY, rows)
        for d in (2, 1, 3):
            send("y", index(("y", k)), sy.at[k, (y + d) % NY], ry.at[k, d - 1], y_peer(d))

    def yq(k):
        arrived(index(("y", k)), ry.at[k])
        total = sy[k, y] + ry[k, 0] + ry[k, 1] + ry[k, 2]
        q[k] = total
        sz[k] = total.astype(sz.dtype)
        send("far", index(("far", k)), sz.at[k], rz.at[k], far)

    def zq(k):
        arrived(index(("far", k)), rz.at[k])
        h[k, c, y] = (q[k] + rz[k].astype(F32)).astype(BF16)
        own = h.at[k, c, y]
        for d in (2, 1, 3):
            send("ya", index(("ya", k)), own, own, y_peer(d))

    def ca(k):
        arrived(index(("ya", k)), h.at[k, c, pl.ds(0, NY - 1)])
        own = h.at[k, c]
        send("ca", index(("ca", k)), own, own, partner)

    def ladder_at(group, slot_z):
        return pl.ds((group % NX) * (2 * piece) + slot_z * piece, piece)

    def ladder_rows(k, group, slot_z):
        return lad[k, ladder_at(group, slot_z), :]

    def mm(k):
        arrived(index(("ca", k)), h.at[k, 1 - c])
        lad[k] = jnp.dot(h[k].reshape(kl, rows), t2[...], preferred_element_type=F32)
        for way in range(2):
            xas[k, way] = ladder_rows(k, x + 2, way).astype(BF16)
            send("a", index(("a", k, way)), xas.at[k, way], xa.at[k, way], x_peer(way))

    def bf(k):
        for way in range(2):
            xbs[k, 1 - way, way] = ladder_rows(k, x + (1 if way == 0 else 3), 1 - way).astype(BF16)
            for s, at_s in enumerate(cuts(k)):
                send_b(k, 1 - way, way, s, at_s)

    def send_b(k, slot_z, way, s, at_s):
        send("b", index(("b", k, slot_z, s)), xbs.at[k, slot_z, way, :, at_s], xb.at[k, slot_z, way, :, at_s], x_peer(way))

    def bd(k):
        for way in range(2):
            arrived(index(("a", k, way)), xa.at[k, way])
        for s, at_s in enumerate(cuts(k)):
            for way in range(2):
                mine = lad[k, ladder_at(x + (1 if way == 0 else 3), way), at_s]
                xbs[k, way, way, :, at_s] = (mine + xa[k, way, :, at_s].astype(F32)).astype(BF16)
                send_b(k, way, way, s, at_s)

    def bs(k):
        for s, at_s in enumerate(cuts(k)):
            for slot_z in range(2):
                arrived(index(("b", k, slot_z, s)), xb.at[k, slot_z, :, :, at_s])
                at_x = ladder_at(x, slot_z)
                total = lad[k, at_x, at_s] + xb[k, slot_z, 0, :, at_s].astype(F32) + xb[k, slot_z, 1, :, at_s].astype(F32)
                if k % 2 == 0:
                    lad[k, at_x, at_s] = total
                zs[k, slot_z, :, at_s] = total.astype(BF16)
            for d in (2,) if k % 2 == 0 else (1, 3):
                send(
                    "zr", index(("zr", k // 2)), zs.at[k, ((z + d) % NZ) // 2, :, at_s],
                    zb.at[k // 2, d - 1, :, at_s], z_peer(d),
                )

    def ou(j):
        arrived(index(("zr", j)), zb.at[j])
        total = ladder_rows(2 * j, x, zz)
        for d in range(3):
            total += zb[j, d].astype(F32)
        out_ref[pl.ds(j * piece, piece), :] = total.astype(BF16)

    events = dict(oa=oa, ob=ob, tt=tt, ox=ox, f1=f1, f2=f2, f3=f3, rl=rl, ma=ma, ys=ys, yq=yq, zq=zq, ca=ca, mm=mm, bf=bf, bd=bd, bs=bs, ou=ou)
    for name in words:
        with jax.named_scope(name):
            events[name[:2]](int(name[2:]))
    with jax.named_scope("drain"):
        sent = dict(
            x=g.at[pl.ds(0, 6)], z=zb, c=rc, y=ry, far=rz, ya=h.at[pl.ds(0, 3)], ca=h.at[pl.ds(0, 4)], a=xa, b=xb, zr=zb
        )
        for kind in kinds:
            waiting(kind, 0, sent[kind]).wait_send()


def on_device(t2_amps, l2_amps):
    rows, width = t2_amps.shape
    piece = l2_amps.shape[0] // PARTS
    kl = NX * 2 * piece
    return pl.pallas_call(
        kernel,
        out_shape=pltpu.VMEM(l2_amps.shape, BF16),
        in_specs=[pl.BlockSpec(memory_space=pl.ANY)] * 2,
        out_specs=pl.BlockSpec(memory_space=pltpu.VMEM),
        scratch_shapes=[
            pltpu.VMEM((rows, width), BF16),
            pltpu.VMEM((width, rows), BF16),
            pltpu.VMEM((CHUNKS, NX, 2, piece, width), BF16),
            pltpu.VMEM((CHUNKS, kl, rows), F32),
            pltpu.VMEM((CHUNKS, kl // 2, rows), F32),
            pltpu.VMEM((CHUNKS, NY, kl // 2 // NY, rows), F32),
            pltpu.VMEM((CHUNKS, NY - 1, kl // 2 // NY, rows), F32),
            pltpu.VMEM((CHUNKS, kl // 2 // NY, rows), F32),
            pltpu.VMEM((CHUNKS, kl // 2 // NY, rows), FAR_TYPE),
            pltpu.VMEM((CHUNKS, kl // 2 // NY, rows), FAR_TYPE),
            pltpu.VMEM((CHUNKS, 2, NY, kl // 2 // NY, rows), BF16),
            pltpu.VMEM((CHUNKS, kl, width), F32),
            pltpu.VMEM((CHUNKS, 2, piece, width), BF16),
            pltpu.VMEM((CHUNKS, 2, piece, width), BF16),
            pltpu.VMEM((CHUNKS, 2, 2, piece, width), BF16),
            pltpu.VMEM((CHUNKS, 2, 2, piece, width), BF16),
            pltpu.VMEM((CHUNKS, 2, piece, width), BF16),
            pltpu.VMEM((PARTS, NZ - 1, piece, width), BF16),
            pltpu.SemaphoreType.DMA((1 + PARTS,)),
            pltpu.SemaphoreType.DMA((10,)),
            pltpu.SemaphoreType.DMA((CHUNKS * 14 + 2,)),
        ],
        compiler_params=pltpu.CompilerParams(
            collective_id=0, has_side_effects=True, vmem_limit_bytes=52 * 2**20
        ),
    )(*(pltpu.with_memory_space_constraint(v, pltpu.HBM) for v in (t2_amps, l2_amps)))


def solution(mesh):
    return jax.shard_map(
        on_device,
        mesh=mesh,
        in_specs=(P("row", "col"), P("row", "col")),
        out_specs=P("row", "col"),
        check_vma=False,
    )
```

```python
import jax
import jax.numpy as jnp
from jax import lax
from jax.experimental import pallas as pl
from jax.experimental.pallas import tpu as pltpu
from jax.sharding import PartitionSpec as P

MESH = pl.DeviceIdType.MESH
F32, BF16 = jnp.float32, jnp.bfloat16

PARTS = 4
CHUNKS = 2 * PARTS
NX, NZ, NY = 4, 4, 4
FAR_TYPE = BF16

ORDER = (
    "ob1 ox1 ox2 ox0",
    "ox3 tt1 ob0 tt0",
    "f11 oa3 f31 oa0",
    "f10 f30 oa1 rl3",
    "tt3 tt2 f23 oa2",
    "rl1 f20 ma3 rl6",
    "ob2 f21 ys3 ma1",
    "ob3 rl0 f22 ys1",
    "ma6 rl2 f12 yq3",
    "ys6 f32 ma0 rl4",
    "f33 f13 yq1 ys0",
    "ma2 yq6 zq3 ys2",
    "rl5 ma4 zq1 yq0",
    "rl7 ys4 ca3 ma5",
    "zq6 mm3 bf3 ca1",
    "yq2 ys5 ma7 yq4",
    "mm1 zq0 ca6 ys7",
    "bf1 bd3 mm6 yq5",
    "zq2 bd1 ca0 bf6",
    "zq4 mm0 yq7 bs3",
    "ca2 bf0 bd6 ca4",
    "bs1 zq5 mm2 bd0",
    "mm4 bf4 zq7 bs6",
    "ca5 bd2 mm5 bs0",
    "bf2 bd4 ca7 mm7",
    "bd5 bs2 bf5 bf7",
    "bs4 bd7 bs5 ou0",
    "ou1 bs7 ou2 ou3",
)


def kernel(
    t2_hbm, l2_hbm, out_ref,
    t2, t2t, g, p, rc, sy, ry, q, sz, rz, h, lad, xas, xa, xbs, xb, zs, zb,
    local, send_sems, sems,
):
    rows, width = t2.shape
    piece = g.shape[3]
    kl = p.shape[1]
    half = kl // 2
    row, col = lax.axis_index("row"), lax.axis_index("col")
    x, z = row // NZ, row % NZ
    zz = z // 2
    y, zh, c = col // 4, (col // 2) % 2, col % 2

    def z_peer(d):
        return (x * NZ + (z + d) % NZ, col)

    def x_peer(way):
        return (((x + (1 if way == 0 else NX - 1)) % NX) * NZ + z, col)

    def y_peer(d):
        return (row, ((y + d) % NY) * 4 + zh * 2 + c)

    far = (row, y * 4 + (1 - zh) * 2 + c)
    partner = (row, y * 4 + zh * 2 + (1 - c))

    loads = []
    for j in range(PARTS):
        loads.append(pltpu.make_async_copy(l2_hbm.at[pl.ds(j * piece, piece)], g.at[2 * j, x, zz], local.at[j]))
    loads.append(pltpu.make_async_copy(t2_hbm, t2, local.at[PARTS]))
    for copy in loads:
        copy.start()

    barrier = pltpu.get_barrier_semaphore()
    peers = [z_peer(1), z_peer(2), z_peer(3), x_peer(0), x_peer(1), y_peer(1), y_peer(2), y_peer(3), far, partner]
    for peer in peers:
        pl.semaphore_signal(barrier, inc=1, device_id=peer, device_id_type=MESH)
    pl.semaphore_wait(barrier, len(peers))

    names = {}

    words = " ".join(ORDER).split()
    last = max(range(CHUNKS), key=lambda k: words.index(f"bs{k}"))
    count = [0]

    def cuts(k):
        n = 3 if k == last else 1
        return [pl.ds(s * (width // n), width // n) for s in range(n)]

    def index(name, size=1):
        if name not in names:
            names[name] = count[0]
            count[0] += size
        return names[name]

    kinds = ("x", "z", "c", "y", "far", "ya", "ca", "a", "b", "zr")

    def send(kind, k, src, dst, device):
        pltpu.make_async_remote_copy(
            src_ref=src, dst_ref=dst, send_sem=send_sems.at[kinds.index(kind)], recv_sem=sems.at[k],
            device_id=device, device_id_type=MESH,
        ).start()

    def waiting(kind, k, ref):
        return pltpu.make_async_remote_copy(
            src_ref=ref, dst_ref=ref, send_sem=send_sems.at[kinds.index(kind)], recv_sem=sems.at[k],
            device_id=partner, device_id_type=MESH,
        )

    def arrived(k, ref):
        with jax.named_scope("w"):
            waiting("x", k, ref).wait_recv()

    def send_x(k, slot_z):
        block = g.at[k, x, slot_z]
        first = index(("x", k), 3)
        for way in range(2):
            send("x", first + jnp.where(slot_z == way, way, 2), block, block, x_peer(way))

    loaded = set()

    def load(j):
        if j not in loaded:
            loaded.add(j)
            loads[j].wait()

    def to_z(j, d):
        load(j)
        send("z", index(("z", j, d)), g.at[2 * j, x, zz], g.at[2 * j + d % 2, x, zz], z_peer(d))

    def oa(j):
        to_z(j, 2)

    def ob(j):
        to_z(j, 1)
        to_z(j, 3)

    def ox(j):
        load(j)
        send_x(2 * j, zz)

    def from_z(j, d):
        k, slot_z = 2 * j + d % 2, ((z + NZ - d) % NZ) // 2
        arrived(index(("z", j, d)), g.at[k, x, slot_z])
        send_x(k, slot_z)

    def f1(j):
        from_z(j, 1)

    def f2(j):
        from_z(j, 2)

    def f3(j):
        from_z(j, 3)

    def rl(k):
        for way in range(2):
            block = g.at[k, (x + (NX - 1 if way == 0 else 1)) % NX, way]
            arrived(index(("x", k), 3) + way, block)
            send("x", index(("x", k), 3) + 2, block, block, x_peer(way))

    def ma(k):
        arrived(index(("x", k), 3) + 2, g.at[k, pl.ds(0, 2)])
        columns = rows // 2
        for s in range(2):
            at_s = pl.ds(s * columns, columns)
            p[k, :, at_s] = jnp.dot(g[k].reshape(kl, width), t2t[:, at_s], preferred_element_type=F32)
            send("c", index(("c", k)), p.at[k, pl.ds((1 - c) * half, half), at_s], rc.at[k, :, at_s], partner)

    def tt(i):
        load(PARTS)
        size = rows // 4
        t2t[:, i * size : (i + 1) * size] = t2[i * size : (i + 1) * size, :].T

    def ys(k):
        arrived(index(("c", k)), rc.at[k])
        sy[k] = (p[k, pl.ds(c * half, half), :] + rc[k]).reshape(NY, half // NY, rows)
        for d in (2, 1, 3):
            send("y", index(("y", k)), sy.at[k, (y + d) % NY], ry.at[k, d - 1], y_peer(d))

    def yq(k):
        arrived(index(("y", k)), ry.at[k])
        total = sy[k, y] + ry[k, 0] + ry[k, 1] + ry[k, 2]
        q[k] = total
        sz[k] = total.astype(sz.dtype)
        send("far", index(("far", k)), sz.at[k], rz.at[k], far)

    def zq(k):
        arrived(index(("far", k)), rz.at[k])
        h[k, c, y] = (q[k] + rz[k].astype(F32)).astype(BF16)
        own = h.at[k, c, y]
        for d in (2, 1, 3):
            send("ya", index(("ya", k)), own, own, y_peer(d))

    def ca(k):
        arrived(index(("ya", k)), h.at[k, c, pl.ds(0, NY - 1)])
        own = h.at[k, c]
        send("ca", index(("ca", k)), own, own, partner)

    def ladder_at(group, slot_z):
        return pl.ds((group % NX) * (2 * piece) + slot_z * piece, piece)

    def ladder_rows(k, group, slot_z):
        return lad[k, ladder_at(group, slot_z), :]

    def mm(k):
        arrived(index(("ca", k)), h.at[k, 1 - c])
        lad[k] = jnp.dot(h[k].reshape(kl, rows), t2[...], preferred_element_type=F32)
        for way in range(2):
            xas[k, way] = ladder_rows(k, x + 2, way).astype(BF16)
            send("a", index(("a", k, way)), xas.at[k, way], xa.at[k, way], x_peer(way))

    def bf(k):
        for way in range(2):
            xbs[k, 1 - way, way] = ladder_rows(k, x + (1 if way == 0 else 3), 1 - way).astype(BF16)
            for s, at_s in enumerate(cuts(k)):
                send_b(k, 1 - way, way, s, at_s)

    def send_b(k, slot_z, way, s, at_s):
        send("b", index(("b", k, slot_z, s)), xbs.at[k, slot_z, way, :, at_s], xb.at[k, slot_z, way, :, at_s], x_peer(way))

    def bd(k):
        for way in range(2):
            arrived(index(("a", k, way)), xa.at[k, way])
        for s, at_s in enumerate(cuts(k)):
            for way in range(2):
                mine = lad[k, ladder_at(x + (1 if way == 0 else 3), way), at_s]
                xbs[k, way, way, :, at_s] = (mine + xa[k, way, :, at_s].astype(F32)).astype(BF16)
                send_b(k, way, way, s, at_s)

    def bs(k):
        for s, at_s in enumerate(cuts(k)):
            for slot_z in range(2):
                arrived(index(("b", k, slot_z, s)), xb.at[k, slot_z, :, :, at_s])
                at_x = ladder_at(x, slot_z)
                total = lad[k, at_x, at_s] + xb[k, slot_z, 0, :, at_s].astype(F32) + xb[k, slot_z, 1, :, at_s].astype(F32)
                if k % 2 == 0:
                    lad[k, at_x, at_s] = total
                zs[k, slot_z, :, at_s] = total.astype(BF16)
            for d in (2,) if k % 2 == 0 else (1, 3):
                send(
                    "zr", index(("zr", k // 2)), zs.at[k, ((z + d) % NZ) // 2, :, at_s],
                    zb.at[k // 2, d - 1, :, at_s], z_peer(d),
                )

    def ou(j):
        arrived(index(("zr", j)), zb.at[j])
        total = ladder_rows(2 * j, x, zz)
        for d in range(3):
            total += zb[j, d].astype(F32)
        out_ref[pl.ds(j * piece, piece), :] = total.astype(BF16)

    events = dict(oa=oa, ob=ob, tt=tt, ox=ox, f1=f1, f2=f2, f3=f3, rl=rl, ma=ma, ys=ys, yq=yq, zq=zq, ca=ca, mm=mm, bf=bf, bd=bd, bs=bs, ou=ou)
    for name in words:
        with jax.named_scope(name):
            events[name[:2]](int(name[2:]))
    with jax.named_scope("drain"):
        sent = dict(
            x=g.at[pl.ds(0, 6)], z=zb, c=rc, y=ry, far=rz, ya=h.at[pl.ds(0, 3)], ca=h.at[pl.ds(0, 4)], a=xa, b=xb, zr=zb
        )
        for kind in kinds:
            waiting(kind, 0, sent[kind]).wait_send()


def on_device(t2_amps, l2_amps):
    rows, width = t2_amps.shape
    piece = l2_amps.shape[0] // PARTS
    kl = NX * 2 * piece
    return pl.pallas_call(
        kernel,
        out_shape=pltpu.VMEM(l2_amps.shape, BF16),
        in_specs=[pl.BlockSpec(memory_space=pl.ANY)] * 2,
        out_specs=pl.BlockSpec(memory_space=pltpu.VMEM),
        scratch_shapes=[
            pltpu.VMEM((rows, width), BF16),
            pltpu.VMEM((width, rows), BF16),
            pltpu.VMEM((CHUNKS, NX, 2, piece, width), BF16),
            pltpu.VMEM((CHUNKS, kl, rows), F32),
            pltpu.VMEM((CHUNKS, kl // 2, rows), F32),
            pltpu.VMEM((CHUNKS, NY, kl // 2 // NY, rows), F32),
            pltpu.VMEM((CHUNKS, NY - 1, kl // 2 // NY, rows), F32),
            pltpu.VMEM((CHUNKS, kl // 2 // NY, rows), F32),
            pltpu.VMEM((CHUNKS, kl // 2 // NY, rows), FAR_TYPE),
            pltpu.VMEM((CHUNKS, kl // 2 // NY, rows), FAR_TYPE),
            pltpu.VMEM((CHUNKS, 2, NY, kl // 2 // NY, rows), BF16),
            pltpu.VMEM((CHUNKS, kl, width), F32),
            pltpu.VMEM((CHUNKS, 2, piece, width), BF16),
            pltpu.VMEM((CHUNKS, 2, piece, width), BF16),
            pltpu.VMEM((CHUNKS, 2, 2, piece, width), BF16),
            pltpu.VMEM((CHUNKS, 2, 2, piece, width), BF16),
            pltpu.VMEM((CHUNKS, 2, piece, width), BF16),
            pltpu.VMEM((PARTS, NZ - 1, piece, width), BF16),
            pltpu.SemaphoreType.DMA((1 + PARTS,)),
            pltpu.SemaphoreType.DMA((10,)),
            pltpu.SemaphoreType.DMA((CHUNKS * 14 + 4,)),
        ],
        compiler_params=pltpu.CompilerParams(
            collective_id=0, has_side_effects=True, vmem_limit_bytes=52 * 2**20
        ),
    )(*(pltpu.with_memory_space_constraint(v, pltpu.HBM) for v in (t2_amps, l2_amps)))


def solution(mesh):
    return jax.shard_map(
        on_device,
        mesh=mesh,
        in_specs=(P("row", "col"), P("row", "col")),
        out_specs=P("row", "col"),
        check_vma=False,
    )
```
